32 devices in a mesh: tm: 8 (over y, x, core), space: 4 (over z).
Axes of the slice: x: 2, y: 2, z: 4, core: 2. Of those that a mesh axis runs over, the one named last changes fastest.
Arguments:
- initial_density: float32 [96, 512], P('space'), may hold values from 0.5 to 2
- terminal_cost: float32 [96, 512], P('space'), may hold values from -1.2 to 1.2
- running_cost: float32 [96, 512], P('space'), may hold values from -0.3 to 0.3
- discount_rate: float32 [96, 512], P('space'), may hold values from 0.003 to 0.5
- slice_steps: int32 [8], replicated, may hold values from 4 to 8
Outputs:
- density_path: float32 [8, 96, 512], P('tm', 'space')
- value_path: float32 [8, 96, 512], P('tm', 'space')
The draws below stay inside these ranges and needn't reach their ends.
All inputs are finite; a program needn't handle non-finite values.
Results may differ from the reference program's by a relative error of at most 0.0003.
Values sent between devices are 32-bit elements; how exact they have to be, the bound alone decides.
A program may use at most 64 MiB of HBM per device.

```python
import math
import jax
import jax.numpy as jnp
from jax import lax

NY = 512
K = 8
ITERS = 2
SLICES = 8
NX = 96


def plant(array, stream_key, least, high):
    extent = array.shape
    index_at = [jax.random.randint(jax.random.fold_in(stream_key, axis), (), 0, extent[axis]) for axis in range(len(extent))]
    array = array.at[tuple(index_at)].set(least)
    longest = extent.index(max(extent))
    index_at[longest] = (index_at[longest] + 1) % extent[longest]
    return array.at[tuple(index_at)].set(high)


def block_levels(rng, shape, cuts, low, top_value):
    level = 1.0
    for dim, blocks in cuts:
        steps = jax.random.uniform(jax.random.fold_in(jax.random.fold_in(rng, 6), dim), (blocks,), jnp.float32, low / len(cuts), top_value / len(cuts))
        level = level * jnp.repeat(jnp.exp(steps), shape[dim] // blocks).reshape((-1,) + (1,) * (len(shape) - 1 - dim))
    return level


def gaussian(key, extent, spread, most, split=(), dtype=jnp.bfloat16):
    loudness = block_levels(key, extent, split, -0.22, 0.18) if split else 1.0
    drawn = jax.random.normal(key, extent, jnp.float32) * spread * loudness
    return jnp.minimum(jnp.maximum(drawn, -most), most).astype(dtype)


def setup_inputs(seed: int = 0) -> dict:
    splits = jax.random.split(jax.random.key(seed), 6)
    return {
        "initial_density": jnp.clip(jnp.exp(math.log(2.0) - 1.3862944 * jax.random.uniform(splits[0], (NX, NY), jnp.float32) ** block_levels(splits[0], (NX, NY), ((0, 4),), -0.2, 0.2)), 0.5, 2.0),
        "terminal_cost": gaussian(splits[1], (NX, NY), 0.2, 1.2, ((0, 4),), jnp.float32),
        "running_cost": gaussian(splits[2], (NX, NY), 0.05, 0.3, ((0, 4),), jnp.float32),
        "discount_rate": jnp.clip(jnp.exp(math.log(0.5) - 5.115996 * jax.random.uniform(splits[3], (NX, NY), jnp.float32) ** block_levels(splits[3], (NX, NY), ((0, 4),), -0.2, 0.2)), 0.003, 0.5),
        "slice_steps": plant(jax.random.randint(splits[4], (SLICES,), 4, K + 1), jax.random.fold_in(splits[4], 1), 4, K).astype(jnp.int32),
    }


time_step = 0.05
diffusion = 2.0
coupling = 0.1


def laplace(padded):
    middle = padded[1:-1]
    return padded[2:] + padded[:-2] + jnp.roll(middle, 1, 1) + jnp.roll(middle, -1, 1) - 4.0 * middle


def slopes(padded):
    middle = padded[1:-1]
    return 0.5 * (padded[2:] - padded[:-2]), 0.5 * (jnp.roll(middle, -1, 1) - jnp.roll(middle, 1, 1))


def value_step(padded, source):
    slope_across, slope_along = slopes(padded)
    hamilton = 0.5 * (slope_across * slope_across + slope_along * slope_along)
    return padded[1:-1] + time_step * (diffusion * laplace(padded) - hamilton + source)


def density_step(density, value):
    slope_across, slope_along = slopes(value)
    flux_across = density * slope_across
    flux_along = density * slope_along
    inner = flux_along[1:-1]
    divergence = 0.5 * (flux_across[2:] - flux_across[:-2]) + 0.5 * (jnp.roll(inner, -1, 1) - jnp.roll(inner, 1, 1))
    return density[1:-1] + time_step * (diffusion * laplace(density) + divergence)


def wrap_rows(field, width):
    return jnp.concatenate([field[-width:], field, field[:width]], axis=0)


def fine_solve(density_start, value_end, running_cost, steps):
    source = running_cost + coupling * density_start
    value_now = value_end
    stored = [value_now]
    for substep in range(K):
        active = substep >= K - steps
        value_now = jnp.where(active, value_step(wrap_rows(value_now, 1), source), value_now)
        stored.append(value_now)
    density_now = density_start
    for substep in range(K):
        active = substep < steps
        density_now = jnp.where(active, density_step(wrap_rows(density_now, 1), wrap_rows(stored[K - substep], 2)), density_now)
    return density_now, value_now


def reference(initial_density, terminal_cost, running_cost, discount_rate, slice_steps):
    steps_float = slice_steps.astype(jnp.float32)
    factors = [jnp.exp(-discount_rate * (time_step * steps_float[number])) for number in range(SLICES)]
    reliefs = [-jnp.expm1(-discount_rate * (time_step * steps_float[number])) / discount_rate * running_cost for number in range(SLICES)]
    densities = [initial_density]
    for number in range(SLICES - 1):
        densities.append(factors[number] * densities[number])
    values = [terminal_cost] * SLICES
    for number in range(SLICES - 2, -1, -1):
        values[number] = factors[number + 1] * values[number + 1] + reliefs[number + 1]
    for iteration in range(ITERS):
        fine_density, fine_value = lax.map(
            lambda item: fine_solve(item[0], item[1], running_cost, item[2]),
            (jnp.stack(densities), jnp.stack(values), slice_steps))
        density_terms = [fine_density[number] - factors[number] * densities[number] for number in range(SLICES)]
        value_terms = [fine_value[number] - factors[number] * values[number] for number in range(SLICES)]
        new_densities = [initial_density]
        for number in range(SLICES - 1):
            new_densities.append(factors[number] * new_densities[number] + density_terms[number])
        new_values = [terminal_cost] * SLICES
        for number in range(SLICES - 2, -1, -1):
            new_values[number] = factors[number + 1] * new_values[number + 1] + value_terms[number + 1]
        densities = new_densities
        values = new_values
    return jnp.stack(densities), jnp.stack(values)
```

```python
import functools

import jax
import jax.numpy as jnp
from jax import lax
from jax.experimental import pallas as pl
from jax.experimental.pallas import tpu as pltpu
from jax.sharding import PartitionSpec as P

K = 8
ITERS = 2
TIME_STEP = 0.05
DIFFUSION = 2.0
COUPLING = 0.1
REACH = 24
MARGIN = 16
INNER = 8
MESH = pl.DeviceIdType.MESH


def shifted(field, dim):
    size = field.shape[dim]
    return pltpu.roll(field, 1, dim), pltpu.roll(field, size - 1, dim)


def rise(field, dim):
    before, after = shifted(field, dim)
    return after - before


def grown(exponent, power):
    series = 1.0 + exponent * (1.0 / 8.0)
    for order in range(7, 1, -1):
        series = 1.0 + exponent * (1.0 / order) * series
    return jnp.where(jnp.abs(exponent) < 0.35, exponent * series, power - 1.0)


def value_step(value, source, dt):
    up, down = shifted(value, 0)
    left, right = shifted(value, 1)
    across, along = down - up, right - left
    k = dt * DIFFUSION
    total = (up + down) + (left + right)
    hamilton = across * across + along * along
    new = value * (1.0 - 4.0 * k) + (k * total + dt * (source - 0.125 * hamilton))
    return new, across, along


def density_step(density, across, along, dt):
    k, kk = dt * DIFFUSION, dt * 0.25
    pa, pb = kk * across, kk * along
    size = density.shape
    return (
        density * (1.0 - 4.0 * k)
        + (pltpu.roll(density * (k + pa), size[0] - 1, 0) + pltpu.roll(density * (k - pa), 1, 0))
        + (pltpu.roll(density * (k + pb), size[1] - 1, 1) + pltpu.roll(density * (k - pb), 1, 1))
    )


def kernel(
    n, ring, steps, m0_in, ut_in, rc_in, rate_in, m_out, u_out,
    raw, path, ubuf, source, slopes, dbuf, damp,
    term, pair, chipsum, gathered,
    load_sem, halo_send, halo_recv, path_send, path_recv,
    pair_send, pair_recv, sum_send, sum_recv,
):
    rows, cols = m0_in.shape
    chips = n // 2
    me, place = lax.axis_index("tm"), lax.axis_index("space")
    chip, core = me // 2, me % 2
    partner = chip * 2 + 1 - core
    above, below = lax.rem(place + ring - 1, ring), lax.rem(place + 1, ring)
    own = pl.ds(rows, rows)
    inputs = (m0_in, ut_in, rc_in, rate_in)

    loads = [
        pltpu.make_async_copy(ref, raw.at[f, own], load_sem.at[f]) for f, ref in enumerate(inputs)
    ]
    for load in loads:
        load.start()

    barrier = pltpu.get_barrier_semaphore()
    pl.semaphore_signal(barrier, inc=1, device_id=(partner, place), device_id_type=MESH)
    for other in (above, below):
        pl.semaphore_signal(barrier, inc=1, device_id=(me, other), device_id_type=MESH)
    for hop in range(1, chips):
        peer = lax.rem(chip + hop, chips) * 2 + core
        pl.semaphore_signal(barrier, inc=1, device_id=(peer, place), device_id_type=MESH)
    pl.semaphore_wait(barrier, 2 + chips)

    def halo(src, dst, send, recv, width):
        return [
            pltpu.make_async_remote_copy(
                src_ref=src.at[pl.ds(rows - width, width)],
                dst_ref=dst.at[pl.ds(rows - width, width)],
                send_sem=send.at[0], recv_sem=recv.at[0],
                device_id=(me, below), device_id_type=MESH,
            ),
            pltpu.make_async_remote_copy(
                src_ref=src.at[pl.ds(0, width)],
                dst_ref=dst.at[pl.ds(2 * rows, width)],
                send_sem=send.at[1], recv_sem=recv.at[1],
                device_id=(me, above), device_id_type=MESH,
            ),
        ]

    first = []
    for f in (3, 1, 2, 0):
        width = MARGIN if f == 0 else REACH
        first += halo(inputs[f], raw.at[f], halo_send.at[f], halo_recv.at[f], width)
    for copy in first:
        copy.start()

    own_steps = steps[me]
    zero = jnp.int32(0)
    before, after = zero, zero
    for j in range(n):
        before = before + jnp.where(j < me, steps[j], 0)
        after = after + jnp.where(j > me, steps[j], 0)

    def lasting(count):
        return TIME_STEP * count.astype(jnp.float32)

    for load in loads:
        load.wait()
    rate_own = raw[3, own]
    for c in range(chips):
        damp[c] = jnp.exp(-rate_own * lasting(steps[2 * c] + steps[2 * c + 1]))
    damp_own = jnp.exp(-rate_own * lasting(own_steps))
    damp_partner = jnp.exp(-rate_own * lasting(steps[partner]))
    damp[chips] = damp_own
    damp[chips + 1] = damp_partner

    for copy in first:
        copy.wait_recv()
    rate = raw[3]
    path[0, 0] = jnp.exp(-rate * lasting(before)) * raw[0]
    gone = -rate * lasting(after)
    kept = jnp.exp(gone)
    path[0, 1] = kept * raw[1] - grown(gone, kept) / rate * raw[2]

    wide = pl.ds(rows - MARGIN, rows + 2 * MARGIN)

    def meet(it, kind):
        return pltpu.make_async_remote_copy(
            src_ref=term.at[it, kind], dst_ref=pair.at[it, kind],
            send_sem=pair_send.at[it, kind], recv_sem=pair_recv.at[it, kind],
            device_id=(partner, place), device_id_type=MESH,
        )

    def spread(it, kind, slot, target):
        return pltpu.make_async_remote_copy(
            src_ref=chipsum.at[it, kind], dst_ref=gathered.at[it, kind, slot],
            send_sem=sum_send.at[it, kind, target], recv_sem=sum_recv.at[it, kind, slot],
            device_id=(target * 2 + core, place), device_id_type=MESH,
        )

    def needs(kind, target):
        return target > chip if kind == 0 else target < chip

    def send_sums(it, kind):
        mine, theirs = term[it, kind], pair[it, kind]
        mine_last = core == (1 if kind == 0 else 0)
        chipsum[it, kind] = jnp.where(
            mine_last, damp[chips] * theirs + mine, damp[chips + 1] * mine + theirs
        )
        for target in range(chips):
            @pl.when(needs(kind, target))
            def _():
                spread(it, kind, chip, target).start()

    def collect(it, kind, into):
        into[...] = raw[kind, own]
        for c in range(chips) if kind == 0 else range(chips - 1, -1, -1):
            @pl.when(c < chip if kind == 0 else c > chip)
            def _():
                spread(it, kind, c, c).wait_recv()
                into[...] = damp[c] * into[...] + gathered[it, kind, c]

        @pl.when(core == (1 if kind == 0 else 0))
        def _():
            into[...] = damp[chips + 1] * into[...] + pair[it, kind]

    for it in range(ITERS):
        last = it == ITERS - 1
        field = raw[2] + COUPLING * path[it, 0]
        source[...] = field[rows - MARGIN : 2 * rows + MARGIN]

        def dt_value(q):
            return jnp.where(q >= K - own_steps, TIME_STEP, 0.0).astype(jnp.float32)

        def dt_density(i):
            return jnp.where(i < own_steps, TIME_STEP, 0.0).astype(jnp.float32)

        new, _, _ = value_step(path[it, 1], field, dt_value(0))
        ubuf[...] = new[rows - MARGIN : 2 * rows + MARGIN]

        cut = slice(MARGIN - INNER, MARGIN + rows + INNER)

        def on_value(q, carry):
            new, across, along = value_step(ubuf[...], source[...], dt_value(q))
            slopes[q - 1, 0] = across[cut]
            slopes[q - 1, 1] = along[cut]
            ubuf[...] = new
            return carry

        lax.fori_loop(1, K, on_value, 0, unroll=K - 1)
        value = ubuf[...]
        term[it, 1] = value[MARGIN : MARGIN + rows] - damp[chips] * path[it, 1, own]
        meet(it, 1).start()
        slopes[K - 1, 0] = rise(value, 0)[cut]
        slopes[K - 1, 1] = rise(value, 1)[cut]

        dbuf[...] = path[it, 0, pl.ds(rows - INNER, rows + 2 * INNER)]

        def on_density(i, carry):
            dbuf[...] = density_step(
                dbuf[...], slopes[K - 1 - i, 0], slopes[K - 1 - i, 1], dt_density(i)
            )
            return carry

        lax.fori_loop(0, K // 2, on_density, 0, unroll=K // 2)
        meet(it, 1).wait_recv()
        send_sums(it, 1)
        lax.fori_loop(K // 2, K, on_density, 0, unroll=K // 2)
        term[it, 0] = dbuf[pl.ds(INNER, rows)] - damp[chips] * path[it, 0, own]
        meet(it, 0).start()

        value_into = u_out.at[0] if last else path.at[it + 1, 1, own]
        collect(it, 1, value_into)
        if not last:
            on_way = halo(value_into, path.at[it + 1, 1], path_send.at[it, 1], path_recv.at[it, 1], REACH)
            for copy in on_way:
                copy.start()
        meet(it, 0).wait_recv()
        send_sums(it, 0)
        density_into = m_out.at[0] if last else path.at[it + 1, 0, own]
        collect(it, 0, density_into)
        if not last:
            more = halo(density_into, path.at[it + 1, 0], path_send.at[it, 0], path_recv.at[it, 0], MARGIN)
            for copy in more:
                copy.start()
            for copy in on_way + more:
                copy.wait()

    for copy in first:
        copy.wait_send()
    for it in range(ITERS):
        for kind in range(2):
            meet(it, kind).wait_send()
            for target in range(chips):
                @pl.when(needs(kind, target))
                def _():
                    spread(it, kind, chip, target).wait_send()


def on_device(n, ring, initial_density, terminal_cost, running_cost, discount_rate, slice_steps):
    rows, cols = initial_density.shape
    chips = n // 2
    f32 = jnp.float32
    tile = jax.ShapeDtypeStruct((1, rows, cols), f32)
    dma = pltpu.SemaphoreType.DMA
    hbm = pl.BlockSpec(memory_space=pl.ANY)
    vmem = pl.BlockSpec(memory_space=pltpu.VMEM)
    density, value = pl.pallas_call(
        functools.partial(kernel, n, ring),
        out_shape=(tile, tile),
        in_specs=[pl.BlockSpec(memory_space=pltpu.SMEM)] + [hbm] * 4,
        out_specs=(vmem, vmem),
        scratch_shapes=[
            pltpu.VMEM((4, 3 * rows, cols), f32),
            pltpu.VMEM((ITERS, 2, 3 * rows, cols), f32),
            pltpu.VMEM((rows + 2 * MARGIN, cols), f32),
            pltpu.VMEM((rows + 2 * MARGIN, cols), f32),
            pltpu.VMEM((K, 2, rows + 2 * INNER, cols), f32),
            pltpu.VMEM((rows + 2 * INNER, cols), f32),
            pltpu.VMEM((chips + 2, rows, cols), f32),
            pltpu.VMEM((ITERS, 2, rows, cols), f32),
            pltpu.VMEM((ITERS, 2, rows, cols), f32),
            pltpu.VMEM((ITERS, 2, rows, cols), f32),
            pltpu.VMEM((ITERS, 2, chips, rows, cols), f32),
            dma((4,)), dma((4, 2)), dma((4, 2)), dma((ITERS, 2, 2)), dma((ITERS, 2, 2)),
            dma((ITERS, 2)), dma((ITERS, 2)), dma((ITERS, 2, chips)), dma((ITERS, 2, chips)),
        ],
        compiler_params=pltpu.CompilerParams(collective_id=0, has_side_effects=True),
    )(slice_steps, initial_density, terminal_cost, running_cost, discount_rate)
    return density, value


def solution(mesh):
    return jax.shard_map(
        functools.partial(on_device, mesh.shape["tm"], mesh.shape["space"]),
        mesh=mesh,
        in_specs=(P("space", None), P("space", None), P("space", None), P("space", None), P()),
        out_specs=(P("tm", "space", None), P("tm", "space", None)),
        check_vma=False,
    )
```

```python
import functools

import jax
import jax.numpy as jnp
from jax import lax
from jax.experimental import pallas as pl
from jax.experimental.pallas import tpu as pltpu
from jax.sharding import PartitionSpec as P

K = 8
TIME_STEP = 0.05
DIFFUSION = 2.0
COUPLING = 0.1
LANES = 128
MARGIN = 16
INNER = 8
MESH = pl.DeviceIdType.MESH


def shifted(field, dim):
    size = field.shape[dim]
    return pltpu.roll(field, 1, dim), pltpu.roll(field, size - 1, dim)


def rise(field, dim):
    before, after = shifted(field, dim)
    return after - before


def grown(exponent, power):
    series = 1.0 + exponent * (1.0 / 8.0)
    for order in range(7, 1, -1):
        series = 1.0 + exponent * (1.0 / order) * series
    return jnp.where(jnp.abs(exponent) < 0.35, exponent * series, power - 1.0)


def value_step(value, source, dt):
    up, down = shifted(value, 0)
    left, right = shifted(value, 1)
    across, along = down - up, right - left
    k = dt * DIFFUSION
    total = (up + down) + (left + right)
    hamilton = across * across + along * along
    new = value * (1.0 - 4.0 * k) + (k * total + dt * (source - 0.125 * hamilton))
    return new, across, along


def density_step(density, across, along, dt):
    k, kk = dt * DIFFUSION, dt * 0.25
    pa, pb = kk * across, kk * along
    size = density.shape
    return (
        density * (1.0 - 4.0 * k)
        + (pltpu.roll(density * (k + pa), size[0] - 1, 0) + pltpu.roll(density * (k - pa), 1, 0))
        + (pltpu.roll(density * (k + pb), size[1] - 1, 1) + pltpu.roll(density * (k - pb), 1, 1))
    )


def kernel(
    n, ring, blocks, offsets, steps, m0_in, ut_in, rc_in, rate_in, m_out, u_out,
    stage, raw, first, path, ubuf, source, slopes, dbuf, damp, group_damp,
    term, chain, total, gathered, final, landing,
    load_sem, halo_send, halo_recv, relay_send, relay_recv,
    sum_send, sum_recv, out_send, out_recv,
):
    rows, cols = m0_in.shape
    groups = n // blocks
    per = n // groups
    wide = 2 * LANES
    me, place = lax.axis_index("tm"), lax.axis_index("space")
    block, group = me // groups, me % groups
    half = group % 2
    partner = me + 1 - 2 * half
    slot_of = {offset: pl.ds(i * rows, rows) for i, offset in enumerate(offsets)}
    own = slot_of[0]
    base = (offsets.index(0) - 1) * rows
    near = pl.ds(base, 3 * rows)
    far_offsets = [offset for offset in offsets if offset != 0]
    inputs = (m0_in, ut_in, rc_in, rate_in)

    loads = []
    for f, ref in enumerate(inputs):
        for i, step in enumerate((0, 1, blocks - 1)):
            columns = pl.ds(pl.multiple_of(lax.rem(block + step, blocks) * LANES, LANES), LANES)
            loads.append(pltpu.make_async_copy(ref.at[:, columns], stage.at[i, f], load_sem.at[i, f]))
    for load in loads:
        load.start()

    barrier = pltpu.get_barrier_semaphore()
    for hop in range(1, n):
        pl.semaphore_signal(
            barrier, inc=1, device_id=(lax.rem(me + hop, n), place), device_id_type=MESH
        )
    for offset in far_offsets:
        pl.semaphore_signal(
            barrier, inc=1, device_id=(me, lax.rem(place + ring - offset, ring)), device_id_type=MESH
        )

    for load in loads:
        load.wait()
    lane = lax.broadcasted_iota(jnp.int32, (rows, LANES), 1)
    for f in range(4):
        raw[f, own, :LANES] = stage[0, f]
        raw[f, own, LANES:] = jnp.where(lane < LANES // 2, stage[1, f], stage[2, f])
    pl.semaphore_wait(barrier, n - 1 + len(far_offsets))

    mine = pl.ds(2 * half, 2)
    other = pl.ds(2 - 2 * half, 2)

    def fetch(i, offset):
        return pltpu.make_async_remote_copy(
            src_ref=raw.at[mine, own], dst_ref=raw.at[mine, slot_of[offset]],
            send_sem=halo_send.at[i], recv_sem=halo_recv.at[i],
            device_id=(me, lax.rem(place + ring - offset, ring)), device_id_type=MESH,
        )

    def relay(i, offset, fields):
        return pltpu.make_async_remote_copy(
            src_ref=raw.at[fields, slot_of[offset]], dst_ref=raw.at[fields, slot_of[offset]],
            send_sem=relay_send.at[i], recv_sem=relay_recv.at[i],
            device_id=(partner, place), device_id_type=MESH,
        )

    for i, offset in reversed(list(enumerate(far_offsets))):
        fetch(i, offset).start()

    def lasting(count):
        return TIME_STEP * count.astype(jnp.float32)

    zero = jnp.int32(0)
    for i, offset in enumerate(far_offsets):
        fetch(i, offset).wait_recv()
        relay(i, offset, mine).start()
    for i, offset in enumerate(far_offsets):
        relay(i, offset, other).wait_recv()

    rate = raw[3]
    ratio = raw[2] / rate
    for c in range(groups):
        count = zero
        for j in range(c * per, (c + 1) * per):
            count = count + steps[j]
        group_damp[c] = jnp.exp(-raw[3, near] * lasting(count))
    for i in range(per):
        number = group * per + i
        before, after = zero, zero
        for j in range(n):
            before = before + jnp.where(j < number, steps[j], 0)
            after = after + jnp.where(j > number, steps[j], 0)
        damp[i] = jnp.exp(-raw[3, near] * lasting(steps[number]))
        first[0, i] = jnp.exp(-rate * lasting(before)) * raw[0]
        gone = -rate * lasting(after)
        kept = jnp.exp(gone)
        first[1, i] = kept * raw[1] - grown(gone, kept) * ratio

    def spread(it, kind, slot, target):
        if it == 0:
            src, dst = total.at[kind], gathered.at[kind, slot]
        else:
            src, dst = final.at[0, kind], final.at[1 + slot, kind]
        return pltpu.make_async_remote_copy(
            src_ref=src, dst_ref=dst,
            send_sem=sum_send.at[it, kind, target], recv_sem=sum_recv.at[it, kind, slot],
            device_id=(block * groups + target, place), device_id_type=MESH,
        )

    def needs(kind, target):
        return target > group if kind == 0 else target < group

    def onward(kind, count):
        return range(count) if kind == 0 else range(count - 1, -1, -1)

    def region(it):
        if it == 0:
            return pl.ds(0, 3 * rows), pl.ds(0, wide)
        return pl.ds(rows, rows), pl.ds(0, LANES)

    def send_totals(it, kind):
        r, l = region(it)
        running = None
        for i in onward(kind, per):
            own_term = term[kind, i, r, l]
            running = own_term if running is None else damp[i, r, l] * running + own_term
        if it == 0:
            total[kind] = running
        else:
            final[0, kind] = running
        for target in range(groups):
            @pl.when(needs(kind, target))
            def _():
                spread(it, kind, target=target, slot=group).start()

    def collect(it, kind):
        r, l = region(it)
        start = chain.at[r, l]
        start[...] = raw[kind, near][r.start : r.start + r.size, : l.size]
        for c in onward(kind, groups):
            @pl.when(c < group if kind == 0 else c > group)
            def _():
                spread(it, kind, slot=c, target=c).wait_recv()
                piece = gathered[kind, c] if it == 0 else final[1 + c, kind]
                start[...] = group_damp[c, r, l] * start[...] + piece
        running = start[...]
        order = list(onward(kind, per))
        for i in order:
            if it == 0:
                path[kind, i] = running
            else:
                landed = landing.at[1 + i, kind, :, pl.ds(0, LANES)]
                landed[...] = running
                number = group * per + i

                @pl.when(number != me)
                def _():
                    deliver(kind, i).start()

                @pl.when(number == me)
                def _():
                    landing[0, kind, :, pl.ds(pl.multiple_of(block * LANES, LANES), LANES)] = landed[...]
            if i != order[-1]:
                running = damp[i, r, l] * running + term[kind, i, r, l]

    def deliver(kind, i):
        columns = pl.ds(pl.multiple_of(block * LANES, LANES), LANES)
        return pltpu.make_async_remote_copy(
            src_ref=landing.at[1 + i, kind, :, pl.ds(0, LANES)],
            dst_ref=landing.at[0, kind, :, columns],
            send_sem=out_send.at[kind, i], recv_sem=out_recv.at[kind, block],
            device_id=(group * per + i, place), device_id_type=MESH,
        )

    def arrival(kind, b):
        return pltpu.make_async_remote_copy(
            src_ref=landing.at[1, kind, :, pl.ds(0, LANES)],
            dst_ref=landing.at[0, kind, :, pl.ds(b * LANES, LANES)],
            send_sem=out_send.at[kind, 0], recv_sem=out_recv.at[kind, b],
            device_id=(partner, place), device_id_type=MESH,
        )

    def dt_value(count, q):
        return jnp.where(q >= K - count, TIME_STEP, 0.0).astype(jnp.float32)

    def dt_density(count, i):
        return jnp.where(i < count, TIME_STEP, 0.0).astype(jnp.float32)

    window = raw.shape[1]
    for it in range(2):
        size = window if it == 0 else rows + 2 * MARGIN
        keep = slice(base, base + 3 * rows) if it == 0 else slice(MARGIN - INNER, MARGIN + rows + INNER)
        deep = 3 * rows if it == 0 else rows + 2 * INNER

        def one_value(i, carry):
            count = steps[group * per + i]
            u = ubuf.at[pl.ds(0, size)]
            src = source.at[pl.ds(0, size)]
            if it == 0:
                field = raw[2] + COUPLING * first[0, i]
                src[...] = field
                new, _, _ = value_step(first[1, i], field, dt_value(count, 0))
                u[...] = new
            else:
                field = raw[2, near] + COUPLING * path[0, i]
                inside = slice(rows - MARGIN, 2 * rows + MARGIN)
                src[...] = field[inside]
                new, _, _ = value_step(path[1, i], field, dt_value(count, 0))
                u[...] = new[inside]

            def on_value(q, carry):
                new, across, along = value_step(u[...], src[...], dt_value(count, q))
                slopes[i, q - 1, 0, :deep] = across[keep]
                slopes[i, q - 1, 1, :deep] = along[keep]
                u[...] = new
                return carry

            lax.fori_loop(1, K, on_value, 0, unroll=K - 1)
            value = u[...]
            slopes[i, K - 1, 0, :deep] = rise(value, 0)[keep]
            slopes[i, K - 1, 1, :deep] = rise(value, 1)[keep]
            if it == 0:
                term[1, i] = value[base : base + 3 * rows] - damp[i] * first[1, i, near]
            else:
                r, l = region(it)
                term[1, i, r, l] = value[MARGIN : MARGIN + rows, :LANES] - damp[i, r, l] * path[1, i, r, l]
            return carry

        lax.fori_loop(0, per, one_value, 0)
        send_totals(it, 1)

        def one_density(i, carry):
            count = steps[group * per + i]
            d = dbuf.at[pl.ds(0, deep)]
            d[...] = first[0, i, near] if it == 0 else path[0, i, pl.ds(rows - INNER, deep)]

            def on_density(q, carry):
                d[...] = density_step(
                    d[...], slopes[i, K - 1 - q, 0, :deep], slopes[i, K - 1 - q, 1, :deep],
                    dt_density(count, q),
                )
                return carry

            lax.fori_loop(0, K, on_density, 0, unroll=K)
            if it == 0:
                term[0, i] = d[...] - damp[i] * first[0, i, near]
            else:
                r, l = region(it)
                density = d[...]
                term[0, i, r, l] = density[INNER : INNER + rows, :LANES] - damp[i, r, l] * path[0, i, r, l]
            return carry

        lax.fori_loop(0, per, one_density, 0)
        send_totals(it, 0)
        collect(it, 1)
        collect(it, 0)

    sender = me // per
    for kind, out in ((1, u_out), (0, m_out)):
        for b in range(blocks):
            @pl.when(b * groups + sender != me)
            def _():
                arrival(kind, b).wait_recv()
        out[0] = landing[0, kind]

    for i, offset in enumerate(far_offsets):
        fetch(i, offset).wait_send()
        relay(i, offset, mine).wait_send()
    for kind in range(2):
        for it in range(2):
            for target in range(groups):
                @pl.when(needs(kind, target))
                def _():
                    spread(it, kind, target=target, slot=group).wait_send()
        for i in range(per):
            @pl.when(group * per + i != me)
            def _():
                deliver(kind, i).wait_send()


def on_device(n, ring, initial_density, terminal_cost, running_cost, discount_rate, slice_steps):
    rows, cols = initial_density.shape
    blocks = cols // LANES
    groups = n // blocks
    per = n // groups
    wide = 2 * LANES
    assert groups % 2 == 0 and groups * blocks == n and blocks >= 3 and rows >= 24
    offsets = (-1, 0, 1, 2) if ring == 4 else (-2, -1, 0, 1, 2)
    assert ring >= 4
    window = len(offsets) * rows
    f32 = jnp.float32
    tile = jax.ShapeDtypeStruct((1, rows, cols), f32)
    dma = pltpu.SemaphoreType.DMA
    hbm = pl.BlockSpec(memory_space=pl.ANY)
    vmem = pl.BlockSpec(memory_space=pltpu.VMEM)
    far = len(offsets) - 1
    return pl.pallas_call(
        functools.partial(kernel, n, ring, blocks, offsets),
        out_shape=(tile, tile),
        in_specs=[pl.BlockSpec(memory_space=pltpu.SMEM)] + [hbm] * 4,
        out_specs=(vmem, vmem),
        scratch_shapes=[
            pltpu.VMEM((3, 4, rows, LANES), f32),
            pltpu.VMEM((4, window, wide), f32),
            pltpu.VMEM((2, per, window, wide), f32),
            pltpu.VMEM((2, per, 3 * rows, wide), f32),
            pltpu.VMEM((window, wide), f32),
            pltpu.VMEM((window, wide), f32),
            pltpu.VMEM((per, K, 2, 3 * rows, wide), f32),
            pltpu.VMEM((3 * rows, wide), f32),
            pltpu.VMEM((per, 3 * rows, wide), f32),
            pltpu.VMEM((groups, 3 * rows, wide), f32),
            pltpu.VMEM((2, per, 3 * rows, wide), f32),
            pltpu.VMEM((3 * rows, wide), f32),
            pltpu.VMEM((2, 3 * rows, wide), f32),
            pltpu.VMEM((2, groups, 3 * rows, wide), f32),
            pltpu.VMEM((1 + groups, 2, rows, LANES), f32),
            pltpu.VMEM((1 + per, 2, rows, cols), f32),
            dma((3, 4)), dma((far,)), dma((far,)), dma((far,)), dma((far,)),
            dma((2, 2, groups)), dma((2, 2, groups)), dma((2, per)), dma((2, blocks)),
        ],
        compiler_params=pltpu.CompilerParams(collective_id=0, has_side_effects=True),
    )(slice_steps, initial_density, terminal_cost, running_cost, discount_rate)


def solution(mesh):
    return jax.shard_map(
        functools.partial(on_device, mesh.shape["tm"], mesh.shape["space"]),
        mesh=mesh,
        in_specs=(P("space", None), P("space", None), P("space", None), P("space", None), P()),
        out_specs=(P("tm", "space", None), P("tm", "space", None)),
        check_vma=False,
    )
```

```python
import functools

import jax
import jax.numpy as jnp
from jax import lax
from jax.experimental import pallas as pl
from jax.experimental.pallas import tpu as pltpu
from jax.sharding import PartitionSpec as P

K = 8
TIME_STEP = 0.05
DIFFUSION = 2.0
COUPLING = 0.1
LANES = 128
MARGIN = 16
INNER = 8
MESH = pl.DeviceIdType.MESH


def shifted(field, dim):
    size = field.shape[dim]
    return pltpu.roll(field, 1, dim), pltpu.roll(field, size - 1, dim)


def rise(field, dim):
    before, after = shifted(field, dim)
    return after - before


def grown(exponent, power):
    series = 1.0 + exponent * (1.0 / 8.0)
    for order in range(7, 1, -1):
        series = 1.0 + exponent * (1.0 / order) * series
    return jnp.where(jnp.abs(exponent) < 0.35, exponent * series, power - 1.0)


def value_step(value, source, dt):
    up, down = shifted(value, 0)
    left, right = shifted(value, 1)
    across, along = down - up, right - left
    k = dt * DIFFUSION
    total = (up + down) + (left + right)
    hamilton = across * across + along * along
    new = value * (1.0 - 4.0 * k) + (k * total + dt * (source - 0.125 * hamilton))
    return new, across, along


def density_step(density, across, along, dt):
    k, kk = dt * DIFFUSION, dt * 0.25
    pa, pb = kk * across, kk * along
    size = density.shape
    return (
        density * (1.0 - 4.0 * k)
        + (pltpu.roll(density * (k + pa), size[0] - 1, 0) + pltpu.roll(density * (k - pa), 1, 0))
        + (pltpu.roll(density * (k + pb), size[1] - 1, 1) + pltpu.roll(density * (k - pb), 1, 1))
    )


def kernel(
    n, ring, blocks, offsets, steps, m0_in, ut_in, rc_in, rate_in, m_out, u_out,
    stage, raw, parcel, first, path, ubuf, source, slopes, dbuf, damp, group_damp,
    term, chain, total, gathered, final, landing,
    load_sem, halo_send, halo_recv, relay_send, relay_recv,
    sum_send, sum_recv, out_send, out_recv,
):
    rows, cols = m0_in.shape
    groups = n // blocks
    per = n // groups
    wide = 2 * LANES
    me, place = lax.axis_index("tm"), lax.axis_index("space")
    block, group = me // groups, me % groups
    half = group % 2
    partner = me + 1 - 2 * half
    slot_of = {offset: pl.ds(i * rows, rows) for i, offset in enumerate(offsets)}
    own = slot_of[0]
    base = (offsets.index(0) - 1) * rows
    near = pl.ds(base, 3 * rows)
    far_offsets = [offset for offset in offsets if offset != 0]
    inputs = (m0_in, ut_in, rc_in, rate_in)

    loads = []
    for f, ref in enumerate(inputs):
        for i, step in enumerate((0, 1, blocks - 1)):
            columns = pl.ds(pl.multiple_of(lax.rem(block + step, blocks) * LANES, LANES), LANES)
            loads.append(pltpu.make_async_copy(ref.at[:, columns], stage.at[i, f], load_sem.at[i, f]))
    for load in loads:
        load.start()

    barrier = pltpu.get_barrier_semaphore()
    for hop in range(1, n):
        pl.semaphore_signal(
            barrier, inc=1, device_id=(lax.rem(me + hop, n), place), device_id_type=MESH
        )
    for offset in far_offsets:
        pl.semaphore_signal(
            barrier, inc=1, device_id=(me, lax.rem(place + ring - offset, ring)), device_id_type=MESH
        )

    for load in loads:
        load.wait()
    lane = lax.broadcasted_iota(jnp.int32, (rows, LANES), 1)
    for f in range(4):
        raw[f, own, :LANES] = stage[0, f]
        raw[f, own, LANES:] = jnp.where(lane < LANES // 2, stage[1, f], stage[2, f])

    central = (lane >= 4 * K) & (lane < LANES - 4 * K)
    for h in range(2):
        for k in range(2):
            parcel[h, k, own] = stage[0, 2 * h + k]
        parcel[h, 2, own] = jnp.where(
            central, pltpu.roll(raw[2 * h + 1, own, LANES:], LANES // 2, 1), raw[2 * h, own, LANES:]
        )
    pl.semaphore_wait(barrier, n - 1 + len(far_offsets))
    mine, other = half, 1 - half

    def fetch(i, offset):
        return pltpu.make_async_remote_copy(
            src_ref=parcel.at[mine, :, own], dst_ref=parcel.at[mine, :, slot_of[offset]],
            send_sem=halo_send.at[i], recv_sem=halo_recv.at[i],
            device_id=(me, lax.rem(place + ring - offset, ring)), device_id_type=MESH,
        )

    def relay(i, offset, fields):
        return pltpu.make_async_remote_copy(
            src_ref=parcel.at[fields, :, slot_of[offset]], dst_ref=parcel.at[fields, :, slot_of[offset]],
            send_sem=relay_send.at[i], recv_sem=relay_recv.at[i],
            device_id=(partner, place), device_id_type=MESH,
        )

    for i, offset in reversed(list(enumerate(far_offsets))):
        fetch(i, offset).start()

    def lasting(count):
        return TIME_STEP * count.astype(jnp.float32)

    zero = jnp.int32(0)
    for i, offset in enumerate(far_offsets):
        fetch(i, offset).wait_recv()
        relay(i, offset, mine).start()
    for i, offset in enumerate(far_offsets):
        relay(i, offset, other).wait_recv()
    for offset in far_offsets:
        slot = slot_of[offset]
        for h in range(2):
            for k in range(2):
                raw[2 * h + k, slot, :LANES] = parcel[h, k, slot]
            raw[2 * h, slot, LANES:] = parcel[h, 2, slot]
            raw[2 * h + 1, slot, LANES:] = pltpu.roll(parcel[h, 2, slot], LANES // 2, 1)

    rate = raw[3]
    ratio = raw[2] / rate
    for c in range(groups):
        count = zero
        for j in range(c * per, (c + 1) * per):
            count = count + steps[j]
        group_damp[c] = jnp.exp(-raw[3, near] * lasting(count))
    for i in range(per):
        number = group * per + i
        before, after = zero, zero
        for j in range(n):
            before = before + jnp.where(j < number, steps[j], 0)
            after = after + jnp.where(j > number, steps[j], 0)
        damp[i] = jnp.exp(-raw[3, near] * lasting(steps[number]))
        first[0, i] = jnp.exp(-rate * lasting(before)) * raw[0]
        gone = -rate * lasting(after)
        kept = jnp.exp(gone)
        first[1, i] = kept * raw[1] - grown(gone, kept) * ratio

    def spread(it, kind, slot, target):
        if it == 0:
            src, dst = total.at[kind], gathered.at[kind, slot]
        else:
            src, dst = final.at[0, kind], final.at[1 + slot, kind]
        return pltpu.make_async_remote_copy(
            src_ref=src, dst_ref=dst,
            send_sem=sum_send.at[it, kind, target], recv_sem=sum_recv.at[it, kind, slot],
            device_id=(block * groups + target, place), device_id_type=MESH,
        )

    def needs(kind, target):
        return target > group if kind == 0 else target < group

    def onward(kind, count):
        return range(count) if kind == 0 else range(count - 1, -1, -1)

    def region(it):
        if it == 0:
            return pl.ds(0, 3 * rows), pl.ds(0, wide)
        return pl.ds(rows, rows), pl.ds(0, LANES)

    def send_totals(it, kind):
        r, l = region(it)
        running = None
        for i in onward(kind, per):
            own_term = term[kind, i, r, l]
            running = own_term if running is None else damp[i, r, l] * running + own_term
        if it == 0:
            total[kind] = running
        else:
            final[0, kind] = running
        for target in range(groups):
            @pl.when(needs(kind, target))
            def _():
                spread(it, kind, target=target, slot=group).start()

    def collect(it, kind):
        r, l = region(it)
        start = chain.at[r, l]
        start[...] = raw[kind, near][r.start : r.start + r.size, : l.size]
        for c in onward(kind, groups):
            @pl.when(c < group if kind == 0 else c > group)
            def _():
                spread(it, kind, slot=c, target=c).wait_recv()
                piece = gathered[kind, c] if it == 0 else final[1 + c, kind]
                start[...] = group_damp[c, r, l] * start[...] + piece
        running = start[...]
        order = list(onward(kind, per))
        for i in order:
            if it == 0:
                path[kind, i] = running
            else:
                landed = landing.at[1 + i, kind, :, pl.ds(0, LANES)]
                landed[...] = running
                number = group * per + i

                @pl.when(number != me)
                def _():
                    deliver(kind, i).start()

                @pl.when(number == me)
                def _():
                    landing[0, kind, :, pl.ds(pl.multiple_of(block * LANES, LANES), LANES)] = landed[...]
            if i != order[-1]:
                running = damp[i, r, l] * running + term[kind, i, r, l]

    def deliver(kind, i):
        columns = pl.ds(pl.multiple_of(block * LANES, LANES), LANES)
        return pltpu.make_async_remote_copy(
            src_ref=landing.at[1 + i, kind, :, pl.ds(0, LANES)],
            dst_ref=landing.at[0, kind, :, columns],
            send_sem=out_send.at[kind, i], recv_sem=out_recv.at[kind, block],
            device_id=(group * per + i, place), device_id_type=MESH,
        )

    def arrival(kind, b):
        return pltpu.make_async_remote_copy(
            src_ref=landing.at[1, kind, :, pl.ds(0, LANES)],
            dst_ref=landing.at[0, kind, :, pl.ds(b * LANES, LANES)],
            send_sem=out_send.at[kind, 0], recv_sem=out_recv.at[kind, b],
            device_id=(partner, place), device_id_type=MESH,
        )

    def dt_value(count, q):
        return jnp.where(q >= K - count, TIME_STEP, 0.0).astype(jnp.float32)

    def dt_density(count, i):
        return jnp.where(i < count, TIME_STEP, 0.0).astype(jnp.float32)

    window = raw.shape[1]
    for it in range(2):
        size = window if it == 0 else rows + 2 * MARGIN
        keep = slice(base, base + 3 * rows) if it == 0 else slice(MARGIN - INNER, MARGIN + rows + INNER)
        deep = 3 * rows if it == 0 else rows + 2 * INNER

        counts = [steps[group * per + i] for i in range(per)]
        u = [ubuf.at[i, pl.ds(0, size)] for i in range(per)]
        src = [source.at[i, pl.ds(0, size)] for i in range(per)]
        d = [dbuf.at[i, pl.ds(0, deep)] for i in range(per)]
        inside = slice(rows - MARGIN, 2 * rows + MARGIN)
        r, l = region(it)

        for i in range(per):
            if it == 0:
                field = raw[2] + COUPLING * first[0, i]
                src[i][...] = field
                new, _, _ = value_step(first[1, i], field, dt_value(counts[i], 0))
                u[i][...] = new
            else:
                field = raw[2, near] + COUPLING * path[0, i]
                src[i][...] = field[inside]
                new, _, _ = value_step(path[1, i], field, dt_value(counts[i], 0))
                u[i][...] = new[inside]

        def on_value(q, carry):
            for i in range(per):
                new, across, along = value_step(u[i][...], src[i][...], dt_value(counts[i], q))
                slopes[i, q - 1, 0, :deep] = across[keep]
                slopes[i, q - 1, 1, :deep] = along[keep]
                u[i][...] = new
            return carry

        lax.fori_loop(1, K, on_value, 0)
        for i in range(per):
            value = u[i][...]
            slopes[i, K - 1, 0, :deep] = rise(value, 0)[keep]
            slopes[i, K - 1, 1, :deep] = rise(value, 1)[keep]
            if it == 0:
                term[1, i] = value[base : base + 3 * rows] - damp[i] * first[1, i, near]
            else:
                term[1, i, r, l] = value[MARGIN : MARGIN + rows, :LANES] - damp[i, r, l] * path[1, i, r, l]
        send_totals(it, 1)

        for i in range(per):
            d[i][...] = first[0, i, near] if it == 0 else path[0, i, pl.ds(rows - INNER, deep)]

        def on_density(q, carry):
            for i in range(per):
                d[i][...] = density_step(
                    d[i][...], slopes[i, K - 1 - q, 0, :deep], slopes[i, K - 1 - q, 1, :deep],
                    dt_density(counts[i], q),
                )
            return carry

        lax.fori_loop(0, K, on_density, 0)
        for i in range(per):
            density = d[i][...]
            if it == 0:
                term[0, i] = density - damp[i] * first[0, i, near]
            else:
                term[0, i, r, l] = density[INNER : INNER + rows, :LANES] - damp[i, r, l] * path[0, i, r, l]
        send_totals(it, 0)
        collect(it, 1)
        collect(it, 0)

    sender = me // per
    for kind, out in ((1, u_out), (0, m_out)):
        for b in range(blocks):
            @pl.when(b * groups + sender != me)
            def _():
                arrival(kind, b).wait_recv()
        out[0] = landing[0, kind]

    for i, offset in enumerate(far_offsets):
        fetch(i, offset).wait_send()
        relay(i, offset, mine).wait_send()
    for kind in range(2):
        for it in range(2):
            for target in range(groups):
                @pl.when(needs(kind, target))
                def _():
                    spread(it, kind, target=target, slot=group).wait_send()
        for i in range(per):
            @pl.when(group * per + i != me)
            def _():
                deliver(kind, i).wait_send()


def on_device(n, ring, initial_density, terminal_cost, running_cost, discount_rate, slice_steps):
    rows, cols = initial_density.shape
    blocks = cols // LANES
    groups = n // blocks
    per = n // groups
    wide = 2 * LANES
    assert groups % 2 == 0 and groups * blocks == n and blocks >= 3 and rows >= 24
    offsets = (-1, 0, 1, 2) if ring == 4 else (-2, -1, 0, 1, 2)
    assert ring >= 4
    window = len(offsets) * rows
    f32 = jnp.float32
    tile = jax.ShapeDtypeStruct((1, rows, cols), f32)
    dma = pltpu.SemaphoreType.DMA
    hbm = pl.BlockSpec(memory_space=pl.ANY)
    vmem = pl.BlockSpec(memory_space=pltpu.VMEM)
    far = len(offsets) - 1
    return pl.pallas_call(
        functools.partial(kernel, n, ring, blocks, offsets),
        out_shape=(tile, tile),
        in_specs=[pl.BlockSpec(memory_space=pltpu.SMEM)] + [hbm] * 4,
        out_specs=(vmem, vmem),
        scratch_shapes=[
            pltpu.VMEM((3, 4, rows, LANES), f32),
            pltpu.VMEM((4, window, wide), f32),
            pltpu.VMEM((2, 3, window, LANES), f32),
            pltpu.VMEM((2, per, window, wide), f32),
            pltpu.VMEM((2, per, 3 * rows, wide), f32),
            pltpu.VMEM((per, window, wide), f32),
            pltpu.VMEM((per, window, wide), f32),
            pltpu.VMEM((per, K, 2, 3 * rows, wide), f32),
            pltpu.VMEM((per, 3 * rows, wide), f32),
            pltpu.VMEM((per, 3 * rows, wide), f32),
            pltpu.VMEM((groups, 3 * rows, wide), f32),
            pltpu.VMEM((2, per, 3 * rows, wide), f32),
            pltpu.VMEM((3 * rows, wide), f32),
            pltpu.VMEM((2, 3 * rows, wide), f32),
            pltpu.VMEM((2, groups, 3 * rows, wide), f32),
            pltpu.VMEM((1 + groups, 2, rows, LANES), f32),
            pltpu.VMEM((1 + per, 2, rows, cols), f32),
            dma((3, 4)), dma((far,)), dma((far,)), dma((far,)), dma((far,)),
            dma((2, 2, groups)), dma((2, 2, groups)), dma((2, per)), dma((2, blocks)),
        ],
        compiler_params=pltpu.CompilerParams(collective_id=0, has_side_effects=True),
    )(slice_steps, initial_density, terminal_cost, running_cost, discount_rate)


def solution(mesh):
    return jax.shard_map(
        functools.partial(on_device, mesh.shape["tm"], mesh.shape["space"]),
        mesh=mesh,
        in_specs=(P("space", None), P("space", None), P("space", None), P("space", None), P()),
        out_specs=(P("tm", "space", None), P("tm", "space", None)),
        check_vma=False,
    )
```
